16 devices in a mesh: dp: 2 (over y, z), sp: 8 (over x, core).
Axes of the slice: x: 4, y: 2, z: 1, core: 2. Of those that a mesh axis runs over, the one named last changes fastest.
The devices are a block of a 4x4x8 slice.
Arguments:
- tokens: bfloat16 [256, 6144], P('dp'), parts along dimension 0
- w_query: bfloat16 [6144, 6144], replicated
- w_key: bfloat16 [6144, 128], replicated
- w_value: bfloat16 [6144, 128], replicated
- w_out: bfloat16 [6144, 6144], P('sp')
- k_cache: bfloat16 [256, 4096, 128], P('dp', 'sp'), parts along dimension 0
- v_cache: bfloat16 [256, 4096, 128], P('dp', 'sp'), parts along dimension 0
- positions: int32 [256], P('dp'), parts along dimension 0
Outputs:
- output 1: bfloat16 [256, 6144], P('dp'), parts along dimension 0
- output 2: bfloat16 [256, 4096, 128], P('dp', 'sp'), parts along dimension 0
- output 3: bfloat16 [256, 4096, 128], P('dp', 'sp'), parts along dimension 0
There are 2 independent parts. The reference program is written for one: setup_inputs(seed, part) draws one part's arguments, and reference() takes and returns one part's arrays. A program takes and returns all parts, laid end to end along the dimension named above; an argument that names none is the same for every part.
All inputs are finite; a program needn't handle non-finite values.
Results may differ from the reference program's by a relative error of at most 0.00432717.
Values are sent between devices in bfloat16 or wider.
A program may use at most 768 MiB of HBM per device.

```python
import jax
import jax.numpy as jnp
import math
from jax import lax

BATCH_ROWS = 128
SEQ_LEN = 4096
D_MODEL = 6144
N_HEADS = 48
HEAD_DIM = 128
GAIN_BLOCK = 32


def setup_inputs(seed: int = 0, part: int = 0) -> dict:
    root = jax.random.key(seed)
    shared = jax.random.split(root, 4)
    local = jax.random.split(jax.random.fold_in(root, part), 5)
    q_width = N_HEADS * HEAD_DIM
    align_scale = (math.log(SEQ_LEN) + 0.5) * HEAD_DIM ** -0.5
    tokens = jax.random.normal(local[0], (BATCH_ROWS, D_MODEL), jnp.float32)
    key_raw = jax.random.normal(shared[1], (D_MODEL, HEAD_DIM), jnp.float32)
    w_query = (jax.random.normal(shared[0], (D_MODEL, q_width), jnp.float32) + align_scale * jnp.tile(key_raw, (1, N_HEADS))) * D_MODEL ** -0.5
    w_key = key_raw * D_MODEL ** -0.5
    w_value = jax.random.normal(shared[2], (D_MODEL, HEAD_DIM), jnp.float32) * D_MODEL ** -0.5
    w_out = jax.random.normal(shared[3], (q_width, D_MODEL), jnp.float32) * q_width ** -0.5
    n_blocks = SEQ_LEN // GAIN_BLOCK
    key_gains = jax.random.uniform(local[1], (BATCH_ROWS, n_blocks, 1, 1), jnp.float32, 0.6, 1.6)
    k_cache = (jax.random.normal(local[2], (BATCH_ROWS, n_blocks, GAIN_BLOCK, HEAD_DIM), jnp.float32) * key_gains).reshape(BATCH_ROWS, SEQ_LEN, HEAD_DIM)
    v_cache = jax.random.normal(local[3], (BATCH_ROWS, SEQ_LEN, HEAD_DIM), jnp.float32)
    positions = jax.random.randint(local[4], (BATCH_ROWS,), SEQ_LEN // 4, SEQ_LEN, jnp.int32)
    positions = positions.at[0].set(SEQ_LEN - 1).at[1].set(SEQ_LEN // 4)
    return dict(tokens=tokens.astype(jnp.bfloat16), w_query=w_query.astype(jnp.bfloat16), w_key=w_key.astype(jnp.bfloat16), w_value=w_value.astype(jnp.bfloat16), w_out=w_out.astype(jnp.bfloat16), k_cache=k_cache.astype(jnp.bfloat16), v_cache=v_cache.astype(jnp.bfloat16), positions=positions)


def reference(tokens, w_query, w_key, w_value, w_out, k_cache, v_cache, positions):
    queries = jnp.dot(tokens, w_query, preferred_element_type=jnp.float32).astype(jnp.bfloat16)
    queries = queries.reshape(BATCH_ROWS, N_HEADS, HEAD_DIM)
    key_new = jnp.dot(tokens, w_key, preferred_element_type=jnp.float32).astype(jnp.bfloat16)
    value_new = jnp.dot(tokens, w_value, preferred_element_type=jnp.float32).astype(jnp.bfloat16)
    slot_ids = jnp.arange(SEQ_LEN)
    hit_mask = (slot_ids[None, :] == positions[:, None])[:, :, None]
    k_upd = jnp.where(hit_mask, key_new[:, None, :], k_cache)
    v_upd = jnp.where(hit_mask, value_new[:, None, :], v_cache)

    def one_row(row_args):
        q_row, k_row, v_row, pos_row = row_args
        scores = jnp.dot(q_row, k_row.T, preferred_element_type=jnp.float32) * HEAD_DIM ** -0.5
        scores = jnp.where(slot_ids[None, :] <= pos_row, scores, -jnp.inf)
        weights = jnp.exp(scores - jnp.max(scores, axis=1, keepdims=True))
        weight_sum = jnp.sum(weights, axis=1)
        value_sum = jnp.dot(weights.astype(jnp.bfloat16), v_row, preferred_element_type=jnp.float32)
        return value_sum / weight_sum[:, None]

    head_outs = lax.map(one_row, (queries, k_upd, v_upd, positions))
    attn_heads = head_outs.astype(jnp.bfloat16).reshape(BATCH_ROWS, N_HEADS * HEAD_DIM)
    attn_out = jnp.dot(attn_heads, w_out, preferred_element_type=jnp.float32).astype(jnp.bfloat16)
    return (attn_out, k_upd, v_upd)
```

```python
import functools
import math

import jax
import jax.numpy as jnp
from jax import lax
from jax.experimental import pallas as pl
from jax.experimental.pallas import tpu as pltpu
from jax.sharding import PartitionSpec as P

MESH = pl.DeviceIdType.MESH
ANY = pl.BlockSpec(memory_space=pl.ANY)
VMEM = pl.BlockSpec(memory_space=pltpu.VMEM)
SMEM = pl.BlockSpec(memory_space=pltpu.SMEM)
F32 = jnp.float32
BF16 = jnp.bfloat16
LIMIT = 60 * 1024 * 1024
CHUNKS = 4
GROUP = 8


def dot_t(a, b):
    return lax.dot_general(a, b, (((1,), (1,)), ((), ())), preferred_element_type=F32)


def project_kernel(n_tiles, depth, x_ref, wq_ref, wk_ref, wv_ref, q_ref, kn_ref, vn_ref, wbuf, kvbuf, wsem, kvsem, ssem, rsem):
    me = lax.axis_index('sp')
    core = lax.rem(me, 2)
    partner = me + 1 - 2 * core
    width = wbuf.shape[2]
    heads = width // q_ref.shape[2]

    def load(tile, slot):
        col = pl.multiple_of((core * n_tiles + tile) * width, width)
        return pltpu.make_async_copy(wq_ref.at[:, pl.ds(col, width)], wbuf.at[slot], wsem.at[slot])

    kv_loads = [pltpu.make_async_copy(w, kvbuf.at[i], kvsem.at[i]) for i, w in enumerate((wk_ref, wv_ref))]
    for tile in range(depth):
        load(tile, tile).start()
    barrier = pltpu.get_barrier_semaphore()
    pl.semaphore_signal(barrier, inc=1, device_id={'sp': partner}, device_id_type=MESH)
    pl.semaphore_wait(barrier, 1)

    def send(tile):
        head = (core * n_tiles + tile) * heads
        block = q_ref.at[pl.ds(head, heads)]
        return pltpu.make_async_remote_copy(block, block, ssem.at[tile], rsem.at[tile], device_id={'sp': partner}, device_id_type=MESH)

    def body(tile, carry):
        slot = lax.rem(tile, depth)
        load(tile, slot).wait()
        out = jnp.dot(x_ref[...], wbuf[slot], preferred_element_type=F32).astype(BF16)
        head = (core * n_tiles + tile) * heads
        for h in range(heads):
            q_ref[head + h] = out[:, h * q_ref.shape[2]:(h + 1) * q_ref.shape[2]]

        @pl.when(tile + depth < n_tiles)
        def _():
            load(tile + depth, slot).start()
        send(tile).start()
        return carry

    lax.fori_loop(0, n_tiles, body, 0)
    for c in kv_loads:
        c.start()
    for c, i, out in zip(kv_loads, range(2), (kn_ref, vn_ref)):
        c.wait()
        out[...] = jnp.dot(x_ref[...], kvbuf[i], preferred_element_type=F32).astype(BF16)

    def finish(tile, carry):
        send(tile).wait_send()
        head = ((1 - core) * n_tiles + tile) * heads
        block = q_ref.at[pl.ds(head, heads)]
        pltpu.make_async_remote_copy(block, block, ssem.at[tile], rsem.at[tile], device_id={'sp': partner}, device_id_type=MESH).wait_recv()
        return carry

    lax.fori_loop(0, n_tiles, finish, 0)


def attend_kernel(n_heads, scale, pos_ref, q_ref, kn_ref, vn_ref, k_ref, v_ref, ko_ref, vo_ref, o_ref, st_ref,
                  kbuf, vbuf, qs, osc, knf, vnf, mst, lst, isem, wsem, osem):
    me = lax.axis_index('sp')
    slots, group, seq, dim = kbuf.shape
    n_rows = pos_ref.shape[0]
    n_blocks = n_rows // group
    first = me * seq
    knf[...] = kn_ref[...].astype(F32)
    vnf[...] = vn_ref[...].astype(F32)
    mst[...] = jnp.zeros_like(mst)
    lst[...] = jnp.zeros_like(lst)

    def rows(i):
        return pl.ds(i * group, group)

    def load(i, s):
        return (pltpu.make_async_copy(k_ref.at[rows(i)], kbuf.at[s], isem.at[0, s]),
                pltpu.make_async_copy(v_ref.at[rows(i)], vbuf.at[s], isem.at[1, s]))

    def store(i, s):
        return (pltpu.make_async_copy(kbuf.at[s], ko_ref.at[rows(i)], wsem.at[0, s]),
                pltpu.make_async_copy(vbuf.at[s], vo_ref.at[rows(i)], wsem.at[1, s]))

    def put(i, s):
        return pltpu.make_async_copy(osc.at[s], o_ref.at[i], osem.at[s])

    ahead = slots // 2
    for i in range(ahead):
        for c in load(i, i):
            c.start()
    lane = lax.broadcasted_iota(jnp.int32, (1, seq), 1)
    lane_b = lax.broadcasted_iota(jnp.int32, (1, n_rows), 1)
    sub = lax.broadcasted_iota(jnp.int32, (16, dim), 0)

    def body(i, carry):
        s = lax.rem(i, slots)
        oslot = lax.rem(i, 2)
        for c in load(i, s):
            c.wait()

        @pl.when(i + ahead < n_blocks)
        def _():
            nxt = lax.rem(i + ahead, slots)

            @pl.when(i + ahead >= slots)
            def _():
                for c in store(i + ahead - slots, nxt):
                    c.wait()
            for c in load(i + ahead, nxt):
                c.start()

        @pl.when(i >= 2)
        def _():
            put(i - 2, oslot).wait()
        qs[...] = q_ref[:, rows(i), :].astype(F32).reshape(qs.shape)
        local = []
        for j in range(group):
            b = i * group + j
            p = pos_ref[b] - first
            local.append(p)
            pc = jnp.clip(p, 0, seq - 1)
            base = pl.multiple_of((pc // 16) * 16, 16)
            hit = (sub == pc - base) & (p >= 0) & (p < seq)
            for new, buf in ((knf, kbuf), (vnf, vbuf)):
                tile = buf[s, j, pl.ds(base, 16), :].astype(F32)
                buf[s, j, pl.ds(base, 16), :] = jnp.where(hit, new[pl.ds(b, 1), :], tile).astype(BF16)
        m_all, l_all = mst[...], lst[...]
        for j in range(group):
            b = i * group + j
            q = qs[pl.ds(j, n_heads, stride=group), :].astype(BF16)
            sc = jnp.where(lane <= local[j], dot_t(q, kbuf[s, j]), -jnp.inf)
            m = jnp.maximum(jnp.max(sc, axis=1, keepdims=True), -1e30)
            w = jnp.exp2((sc - m) * scale)
            l = jnp.sum(w, axis=1, keepdims=True)
            o = jnp.dot(w.astype(BF16), vbuf[s, j], preferred_element_type=F32)
            osc[oslot, pl.ds(j, n_heads, stride=group), :] = o
            m_all = jnp.where(lane_b == b, m * scale, m_all)
            l_all = jnp.where(lane_b == b, l, l_all)
        mst[...] = m_all
        lst[...] = l_all
        for c in store(i, s):
            c.start()
        put(i, oslot).start()
        return carry

    lax.fori_loop(0, n_blocks, body, 0)
    for i in range(n_blocks - slots, n_blocks):
        for c in store(i, i % slots):
            c.wait()
    for i in (n_blocks - 2, n_blocks - 1):
        put(i, i % 2).wait()
    n_dev = st_ref.shape[0]
    per = n_heads // n_dev
    m_all, l_all = mst[...], lst[...]
    for d in range(n_dev):
        st_ref[d, :n_heads] = m_all
        st_ref[d, n_heads:] = jnp.zeros((st_ref.shape[1] - n_heads, n_rows), F32)
        st_ref[d, n_heads:n_heads + per] = l_all[per * d:per * (d + 1)]


def combine_kernel(n_dev, per, st_ref, o_hbm, wo_hbm, y_ref, o_buf, wo, st_in, fac, linv, ob,
                   o_pair, o_r1, o_l1, o_r2, o_l2, y_buf, y_pair, y_r1, y_l1, y_r2, y_l2,
                   lsem, st_s, st_r, os_s, os_r, ys_s, ys_r, ag_s, ag_r):
    me = lax.axis_index('sp')
    n_chips = n_dev // 2
    core = lax.rem(me, 2)
    other = 1 - core
    chip = me // 2
    partner = me + 1 - 2 * core
    rchip, lchip, xchip = (lax.rem(chip + r, n_chips) for r in (1, 3, 2))
    right, left = rchip * 2 + core, lchip * 2 + core
    opposite = xchip * 2 + core
    chunks, n8 = o_buf.shape[0], o_buf.shape[1]
    rows = n8 * GROUP
    n_heads = n_dev * per
    dim = o_buf.shape[-1]
    width = per * dim
    half_o, half_y = o_buf.shape[4] // 2, rows // 2

    load_o = [pltpu.make_async_copy(o_hbm.at[k], o_buf.at[k], lsem.at[k]) for k in range(chunks)]
    load_w = pltpu.make_async_copy(wo_hbm, wo, lsem.at[chunks])
    for c in load_o:
        c.start()
    load_w.start()
    barrier = pltpu.get_barrier_semaphore()
    for r in range(1, n_dev):
        pl.semaphore_signal(barrier, inc=1, device_id={'sp': lax.rem(me + r, n_dev)}, device_id_type=MESH)
    pl.semaphore_wait(barrier, n_dev - 1)

    def remote(src, dst, s, r, dev):
        return pltpu.make_async_remote_copy(src, dst, s, r, device_id={'sp': dev}, device_id_type=MESH)

    stats = []
    for r in range(1, n_dev):
        dev = lax.rem(me + r, n_dev)
        c = remote(st_ref.at[dev], st_in.at[r - 1], st_s.at[r - 1], st_r.at[r - 1], dev)
        c.start()
        stats.append(c)
    for c in stats:
        c.wait_recv()
    mine = st_ref[0, :n_heads]
    top = mine
    for r in range(n_dev - 1):
        top = jnp.maximum(top, st_in[r, :n_heads])
    fac[...] = jnp.concatenate([jnp.exp2(mine - top), jnp.zeros((fac.shape[1] - n_heads, fac.shape[0]), F32)], axis=0).T
    total = jnp.zeros((8, top.shape[1]), F32)
    for d in range(n_dev):
        def term(st, top_d):
            return st[n_heads:n_heads + per] * jnp.exp2(st[per * d:per * (d + 1)] - top_d)
        top_d = top[per * d:per * (d + 1)]
        part = st_ref[d, n_heads:n_heads + per] * jnp.exp2(mine[per * d:per * (d + 1)] - top_d)
        for r in range(n_dev - 1):
            part += term(st_in[r], top_d)
        part = jnp.concatenate([part, jnp.ones((8 - per, top.shape[1]), F32)], axis=0)
        total = jnp.where(me == d, part, total)
    linv[...] = jnp.concatenate([total, jnp.ones((linv.shape[1] - 8, linv.shape[0]), F32)], axis=0).T

    class Reduce:
        def __init__(self, half, pair_src, pair, r1, l1, r2, l2, s, r):
            self.half, self.pair_src, self.pair = half, pair_src, pair
            self.r1, self.l1, self.r2, self.l2, self.s, self.r = r1, l1, r2, l2, s, r

        def copies(self, k):
            h = functools.partial(self.half, k)
            s, r = self.s, self.r
            return dict(
                pair=lambda: remote(self.pair_src(k), self.pair.at[k], s.at[k, 0], r.at[k, 0], partner),
                r1=lambda: remote(h(xchip, 0), self.r1.at[k], s.at[k, 1], r.at[k, 1], right),
                l1=lambda: remote(h(xchip, 1), self.l1.at[k], s.at[k, 2], r.at[k, 2], left),
                r2a=lambda: remote(h(rchip, 1), self.r2.at[k, 1], s.at[k, 3], r.at[k, 3], right),
                l2a=lambda: remote(h(lchip, 0), self.l2.at[k, 0], s.at[k, 4], r.at[k, 4], left),
                r2b=lambda: remote(h(rchip, 0), self.r2.at[k, 0], s.at[k, 5], r.at[k, 5], right),
                l2b=lambda: remote(h(lchip, 1), self.l2.at[k, 1], s.at[k, 6], r.at[k, 6], left),
            )

        def first(self, k, pair_half):
            c = self.copies(k)
            c['pair']().wait_recv()
            for x, g, name in ((xchip, 0, 'r1'), (xchip, 1, 'l1'), (rchip, 1, 'r2a'), (lchip, 0, 'l2a'),
                               (rchip, 0, None), (lchip, 1, None), (chip, 0, None), (chip, 1, None)):
                self.half(k, x, g)[...] += pair_half(k, x, g)[...]
                if name:
                    c[name]().start()

        def second(self, k):
            c = self.copies(k)
            c['r1']().wait_recv()
            self.half(k, rchip, 0)[...] += self.r1[k]
            c['r2b']().start()
            c['l1']().wait_recv()
            self.half(k, lchip, 1)[...] += self.l1[k]
            c['l2b']().start()

        def third(self, k):
            c = self.copies(k)
            for name in ('r2a', 'l2a', 'r2b', 'l2b'):
                c[name]().wait_recv()

        def drain(self, k):
            for c in self.copies(k).values():
                c().wait_send()

    red_o = Reduce(lambda k, x, g: o_buf.at[k, :, x, core, pl.ds(g * half_o, half_o), :],
                   lambda k: o_buf.at[k, :, :, other], o_pair, o_r1, o_l1, o_r2, o_l2, os_s, os_r)
    red_y = Reduce(lambda k, x, g: y_buf.at[k, core, x, pl.ds(g * half_y, half_y), :],
                   lambda k: y_buf.at[k, other], y_pair, y_r1, y_l1, y_r2, y_l2, ys_s, ys_r)

    def o_pair_half(k, x, g):
        return o_pair.at[k, :, x, pl.ds(g * half_o, half_o), :]

    def y_pair_half(k, x, g):
        return y_pair.at[k, x, pl.ds(g * half_y, half_y), :]

    def scale_o(k):
        load_o[k].wait()

        def one(t, carry):
            f = fac[pl.ds(pl.multiple_of(k * rows + t * GROUP, GROUP), GROUP), :]
            for h in range(n_heads):
                x, c, j = h // (2 * per), (h // per) % 2, h % per
                o_buf[k, t, x, c, j * GROUP:(j + 1) * GROUP, :] = o_buf[k, t, x, c, j * GROUP:(j + 1) * GROUP, :] * f[:, h:h + 1]
            return carry
        lax.fori_loop(0, n8, one, 0)
        red_o.copies(k)['pair']().start()

    def project(k):
        red_o.third(k)
        for t in range(n8):
            inv = linv[pl.ds(k * rows + t * GROUP, GROUP), :]
            for j in range(per):
                g, jj = j // (per // 2), j % (per // 2)
                sl = pl.ds(jj * GROUP, GROUP)
                v = (o_buf[k, t, chip, core, j * GROUP:(j + 1) * GROUP, :] + o_r2[k, g, t, sl, :]) + o_l2[k, g, t, sl, :]
                ob[t * GROUP:(t + 1) * GROUP, j * dim:(j + 1) * dim] = v / inv[:, j:j + 1]
        if k == 0:
            load_w.wait()
        a = ob[...].astype(BF16)
        for c in (other, core):
            def one(x, carry):
                col = pl.multiple_of((x * 2 + c) * width, width)
                y_buf[k, c, x] = jnp.dot(a, wo[:, pl.ds(col, width)], preferred_element_type=F32)
                return carry
            lax.fori_loop(0, n_chips, one, 0)
            if c is other:
                red_y.copies(k)['pair']().start()

    def y_block(k, dev, g=None):
        r = pl.ds(k * rows, rows) if g is None else pl.ds(k * rows + g * half_y, half_y)
        return y_ref.at[r, pl.ds(pl.multiple_of(dev * width, width), width)]

    def ag(k):
        s, r = ag_s, ag_r

        def to(block, i, dev):
            return lambda: remote(block, block, s.at[k, i], r.at[k, i], dev)
        return dict(
            own_r=to(y_block(k, me), 0, right), own_l=to(y_block(k, me), 1, left), own_p=to(y_block(k, me), 2, partner),
            fwd_r=to(y_block(k, left, 0), 3, right), fwd_l=to(y_block(k, right, 1), 4, left),
            left_p=to(y_block(k, left), 5, partner), right_p=to(y_block(k, right), 6, partner),
            opp_p0=to(y_block(k, opposite, 0), 7, partner), opp_p1=to(y_block(k, opposite, 1), 8, partner))

    def ag_in(k):
        s, r = ag_s, ag_r
        flip = lambda dev: dev + 1 - 2 * core

        def at(block, i):
            return lambda: remote(block, block, s.at[k, i], r.at[k, i], partner)
        return dict(
            left=at(y_block(k, left), 0), right=at(y_block(k, right), 1), own=at(y_block(k, partner), 2),
            opp0=at(y_block(k, opposite, 0), 3), opp1=at(y_block(k, opposite, 1), 4),
            left_p=at(y_block(k, flip(left)), 5), right_p=at(y_block(k, flip(right)), 6),
            opp_p0=at(y_block(k, flip(opposite), 0), 7), opp_p1=at(y_block(k, flip(opposite), 1), 8))

    def gather_start(k):
        red_y.third(k)
        for g in range(2):
            v = (y_buf[k, core, chip, g * half_y:(g + 1) * half_y, :] + y_r2[k, g]) + y_l2[k, g]
            y_block(k, me, g)[...] = v.astype(BF16)
        c = ag(k)
        for name in ('own_r', 'own_l', 'own_p'):
            c[name]().start()

    def gather_forward(k):
        c, i = ag(k), ag_in(k)
        i['left']().wait_recv()
        c['fwd_r']().start()
        c['left_p']().start()
        i['right']().wait_recv()
        c['fwd_l']().start()
        c['right_p']().start()

    def gather_opposite(k):
        c, i = ag(k), ag_in(k)
        for n in ('0', '1'):
            i['opp' + n]().wait_recv()
            c['opp_p' + n]().start()

    def gather_end(k):
        i = ag_in(k)
        for name in ('own', 'left_p', 'right_p', 'opp_p0', 'opp_p1'):
            i[name]().wait_recv()

    stages = [scale_o, lambda k: red_o.first(k, o_pair_half), red_o.second, project,
              lambda k: red_y.first(k, y_pair_half), red_y.second, gather_start, gather_forward, gather_opposite, gather_end]
    for t in range(chunks + len(stages) - 1):
        for s in reversed(range(len(stages))):
            if 0 <= t - s < chunks:
                stages[s](t - s)
    for c in stats:
        c.wait_send()
    for k in range(chunks):
        red_o.drain(k)
        red_y.drain(k)
        for c in ag(k).values():
            c().wait_send()


def solution(mesh):
    n_dev = mesh.shape['sp']

    def local_step(tokens, w_query, w_key, w_value, w_out, k_cache, v_cache, positions):
        n_rows, seq, dim = k_cache.shape
        d_model, q_width = w_query.shape
        n_heads = q_width // dim
        per = n_heads // n_dev
        width = 2 * dim
        n_tiles = q_width // width // 2
        depth = 3
        chunk = n_rows // CHUNKS
        n8 = chunk // GROUP
        dma = pltpu.SemaphoreType.DMA

        q, k_new, v_new = pl.pallas_call(
            functools.partial(project_kernel, n_tiles, depth),
            name='project',
            out_shape=[jax.ShapeDtypeStruct((n_heads, n_rows, dim), BF16)] + [jax.ShapeDtypeStruct((n_rows, dim), BF16)] * 2,
            in_specs=[VMEM, ANY, ANY, ANY], out_specs=[VMEM] * 3,
            scratch_shapes=[pltpu.VMEM((depth, d_model, width), BF16), pltpu.VMEM((2, d_model, dim), BF16),
                            dma((depth,)), dma((2,)), dma((n_tiles,)), dma((n_tiles,))],
            compiler_params=pltpu.CompilerParams(collective_id=0, has_side_effects=True, vmem_limit_bytes=LIMIT),
        )(tokens, w_query, w_key, w_value)

        slots = 4
        n_blocks = n_rows // GROUP
        k_out, v_out, o_part, stats = pl.pallas_call(
            functools.partial(attend_kernel, n_heads, dim ** -0.5 * math.log2(math.e)),
            name='attend',
            out_shape=[jax.ShapeDtypeStruct(k_cache.shape, BF16), jax.ShapeDtypeStruct(v_cache.shape, BF16),
                       jax.ShapeDtypeStruct((n_blocks, n_heads * GROUP, dim), F32),
                       jax.ShapeDtypeStruct((n_dev, n_heads + 8, n_rows), F32)],
            in_specs=[SMEM, VMEM, VMEM, VMEM, ANY, ANY], out_specs=[ANY, ANY, ANY, VMEM],
            scratch_shapes=[pltpu.VMEM((slots, GROUP, seq, dim), BF16), pltpu.VMEM((slots, GROUP, seq, dim), BF16),
                            pltpu.VMEM((n_heads * GROUP, dim), F32), pltpu.VMEM((2, n_heads * GROUP, dim), F32),
                            pltpu.VMEM((n_rows, dim), F32), pltpu.VMEM((n_rows, dim), F32),
                            pltpu.VMEM((n_heads, n_rows), F32), pltpu.VMEM((n_heads, n_rows), F32),
                            dma((2, slots)), dma((2, slots)), dma((2,))],
            compiler_params=pltpu.CompilerParams(vmem_limit_bytes=LIMIT),
        )(positions, q, k_new, v_new, k_cache, v_cache)

        n_chips = n_dev // 2
        o_view = o_part.reshape(CHUNKS, n8, n_chips, 2, per * GROUP, dim)
        ho, hy, out_w = per * GROUP // 2, chunk // 2, per * dim
        attn_out = pl.pallas_call(
            functools.partial(combine_kernel, n_dev, per),
            name='combine',
            out_shape=jax.ShapeDtypeStruct((n_rows, w_out.shape[1]), BF16),
            in_specs=[VMEM, ANY, ANY], out_specs=VMEM,
            scratch_shapes=[
                pltpu.VMEM(o_view.shape, F32), pltpu.VMEM(w_out.shape, BF16), pltpu.VMEM((n_dev - 1, n_heads + 8, n_rows), F32),
                pltpu.VMEM((n_rows, 128), F32), pltpu.VMEM((n_rows, 128), F32), pltpu.VMEM((chunk, out_w), F32),
                pltpu.VMEM((CHUNKS, n8, n_chips, per * GROUP, dim), F32),
                pltpu.VMEM((CHUNKS, n8, ho, dim), F32), pltpu.VMEM((CHUNKS, n8, ho, dim), F32),
                pltpu.VMEM((CHUNKS, 2, n8, ho, dim), F32), pltpu.VMEM((CHUNKS, 2, n8, ho, dim), F32),
                pltpu.VMEM((CHUNKS, 2, n_chips, chunk, out_w), F32), pltpu.VMEM((CHUNKS, n_chips, chunk, out_w), F32),
                pltpu.VMEM((CHUNKS, hy, out_w), F32), pltpu.VMEM((CHUNKS, hy, out_w), F32),
                pltpu.VMEM((CHUNKS, 2, hy, out_w), F32), pltpu.VMEM((CHUNKS, 2, hy, out_w), F32),
                dma((CHUNKS + 1,)), dma((n_dev - 1,)), dma((n_dev - 1,)),
                dma((CHUNKS, 7)), dma((CHUNKS, 7)), dma((CHUNKS, 7)), dma((CHUNKS, 7)), dma((CHUNKS, 9)), dma((CHUNKS, 9))],
            compiler_params=pltpu.CompilerParams(collective_id=1, has_side_effects=True, vmem_limit_bytes=LIMIT),
        )(stats, o_view, w_out)
        return attn_out, k_out, v_out

    cache_spec = P('dp', 'sp', None)
    return jax.shard_map(local_step, mesh=mesh, in_specs=(P('dp', None), P(), P(), P(), P('sp', None), cache_spec, cache_spec, P('dp')),
                         out_specs=(P('dp', None), cache_spec, cache_spec), check_vma=False)
```

```python
import functools
import math

import jax
import jax.numpy as jnp
from jax import lax
from jax.experimental import pallas as pl
from jax.experimental.pallas import tpu as pltpu
from jax.sharding import PartitionSpec as P

MESH = pl.DeviceIdType.MESH
ANY = pl.BlockSpec(memory_space=pl.ANY)
VMEM = pl.BlockSpec(memory_space=pltpu.VMEM)
SMEM = pl.BlockSpec(memory_space=pltpu.SMEM)
F32 = jnp.float32
BF16 = jnp.bfloat16
MIB = 1024 * 1024
CHUNKS = 2
GROUP = 8


def dot_t(a, b):
    return lax.dot_general(a, b, (((1,), (1,)), ((), ())), preferred_element_type=F32)


def project_kernel(n_tiles, depth, x_ref, wq_ref, wk_ref, wv_ref, q_ref, kn_ref, vn_ref, wbuf, kvbuf, wsem, kvsem, ssem, rsem):
    me = lax.axis_index('sp')
    core = lax.rem(me, 2)
    partner = me + 1 - 2 * core
    width = wbuf.shape[2]
    heads = width // q_ref.shape[2]

    def load(tile, slot):
        col = pl.multiple_of((core * n_tiles + tile) * width, width)
        return pltpu.make_async_copy(wq_ref.at[:, pl.ds(col, width)], wbuf.at[slot], wsem.at[slot])

    kv_loads = [pltpu.make_async_copy(w, kvbuf.at[i], kvsem.at[i]) for i, w in enumerate((wk_ref, wv_ref))]
    for tile in range(depth):
        load(tile, tile).start()
    barrier = pltpu.get_barrier_semaphore()
    pl.semaphore_signal(barrier, inc=1, device_id={'sp': partner}, device_id_type=MESH)
    pl.semaphore_wait(barrier, 1)

    def send(tile):
        head = (core * n_tiles + tile) * heads
        block = q_ref.at[pl.ds(head, heads)]
        return pltpu.make_async_remote_copy(block, block, ssem.at[tile], rsem.at[tile], device_id={'sp': partner}, device_id_type=MESH)

    def body(tile, carry):
        slot = lax.rem(tile, depth)
        load(tile, slot).wait()
        out = jnp.dot(x_ref[...], wbuf[slot], preferred_element_type=F32).astype(BF16)
        head = (core * n_tiles + tile) * heads
        for h in range(heads):
            q_ref[head + h] = out[:, h * q_ref.shape[2]:(h + 1) * q_ref.shape[2]]

        @pl.when(tile + depth < n_tiles)
        def _():
            load(tile + depth, slot).start()
        send(tile).start()
        return carry

    lax.fori_loop(0, n_tiles, body, 0)
    for c in kv_loads:
        c.start()
    for c, i, out in zip(kv_loads, range(2), (kn_ref, vn_ref)):
        c.wait()
        out[...] = jnp.dot(x_ref[...], kvbuf[i], preferred_element_type=F32).astype(BF16)

    def finish(tile, carry):
        send(tile).wait_send()
        head = ((1 - core) * n_tiles + tile) * heads
        block = q_ref.at[pl.ds(head, heads)]
        pltpu.make_async_remote_copy(block, block, ssem.at[tile], rsem.at[tile], device_id={'sp': partner}, device_id_type=MESH).wait_recv()
        return carry

    lax.fori_loop(0, n_tiles, finish, 0)


def attend_kernel(n_heads, scale, pos_ref, q_ref, kn_ref, vn_ref, k_ref, v_ref, ko_ref, vo_ref, o_ref, st_ref,
                  kbuf, vbuf, qs, scs, wts, osc, knf, vnf, mst, lst, isem, wsem, osem):
    me = lax.axis_index('sp')
    slots, group, seq, dim = kbuf.shape
    n_rows = pos_ref.shape[0]
    n_blocks = n_rows // group
    first = me * seq
    knf[...] = kn_ref[...].astype(F32)
    vnf[...] = vn_ref[...].astype(F32)
    mst[...] = jnp.zeros_like(mst)
    lst[...] = jnp.zeros_like(lst)

    def rows(i):
        return pl.ds(i * group, group)

    def load(i, s):
        return (pltpu.make_async_copy(k_ref.at[rows(i)], kbuf.at[s], isem.at[0, s]),
                pltpu.make_async_copy(v_ref.at[rows(i)], vbuf.at[s], isem.at[1, s]))

    def store(i, s):
        return (pltpu.make_async_copy(kbuf.at[s], ko_ref.at[rows(i)], wsem.at[0, s]),
                pltpu.make_async_copy(vbuf.at[s], vo_ref.at[rows(i)], wsem.at[1, s]))

    def put(i, s):
        return pltpu.make_async_copy(osc.at[s], o_ref.at[i], osem.at[s])

    ahead = slots // 2
    for i in range(ahead):
        for c in load(i, i):
            c.start()
    lane = lax.broadcasted_iota(jnp.int32, (1, seq), 1)
    lane_b = lax.broadcasted_iota(jnp.int32, (1, n_rows), 1)
    sub = lax.broadcasted_iota(jnp.int32, (16, dim), 0)

    def body(i, carry):
        s = lax.rem(i, slots)
        oslot = lax.rem(i, 2)
        for c in load(i, s):
            c.wait()

        @pl.when(i + ahead < n_blocks)
        def _():
            nxt = lax.rem(i + ahead, slots)

            @pl.when(i + ahead >= slots)
            def _():
                for c in store(i + ahead - slots, nxt):
                    c.wait()
            for c in load(i + ahead, nxt):
                c.start()

        @pl.when(i >= 2)
        def _():
            put(i - 2, oslot).wait()
        qs[...] = q_ref[:, rows(i), :].astype(F32).reshape(qs.shape)
        local = []
        for j in range(group):
            b = i * group + j
            p = pos_ref[b] - first
            local.append(p)
            pc = jnp.clip(p, 0, seq - 1)
            base = pl.multiple_of((pc // 16) * 16, 16)
            hit = (sub == pc - base) & (p >= 0) & (p < seq)
            for new, buf in ((knf, kbuf), (vnf, vbuf)):
                tile = buf[s, j, pl.ds(base, 16), :].astype(F32)
                buf[s, j, pl.ds(base, 16), :] = jnp.where(hit, new[pl.ds(b, 1), :], tile).astype(BF16)
        for j in range(group):
            q = qs[pl.ds(j, n_heads, stride=group), :].astype(BF16)
            scs[j] = dot_t(q, kbuf[s, j])
        m_all, l_all = mst[...], lst[...]
        for j in range(group):
            b = i * group + j
            sc = jnp.where(lane <= local[j], scs[j], -jnp.inf)
            m = jnp.maximum(jnp.max(sc, axis=1, keepdims=True), -1e30)
            w = jnp.exp2((sc - m) * scale)
            l = jnp.sum(w, axis=1, keepdims=True)
            wts[j] = w.astype(BF16)
            m_all = jnp.where(lane_b == b, m * scale, m_all)
            l_all = jnp.where(lane_b == b, l, l_all)
        for j in range(group):
            osc[oslot, pl.ds(j, n_heads, stride=group), :] = jnp.dot(wts[j], vbuf[s, j], preferred_element_type=F32)
        mst[...] = m_all
        lst[...] = l_all
        for c in store(i, s):
            c.start()
        put(i, oslot).start()
        return carry

    lax.fori_loop(0, n_blocks, body, 0)
    for i in range(n_blocks - slots, n_blocks):
        for c in store(i, i % slots):
            c.wait()
    for i in (n_blocks - 2, n_blocks - 1):
        put(i, i % 2).wait()
    n_dev = st_ref.shape[0]
    per = n_heads // n_dev
    m_all, l_all = mst[...], lst[...]
    for d in range(n_dev):
        st_ref[d, :n_heads] = m_all
        st_ref[d, n_heads:] = jnp.zeros((st_ref.shape[1] - n_heads, n_rows), F32)
        st_ref[d, n_heads:n_heads + per] = l_all[per * d:per * (d + 1)]


def combine_kernel(n_dev, per, st_ref, o_hbm, wo_hbm, y_ref, o_buf, wo, st_in, fac, linv, ob,
                   o_pair, o_r1, o_l1, o_r2, o_l2, y_buf, y_pair, y_r1, y_l1, y_r2, y_l2,
                   lsem, st_s, st_r, os_s, os_r, ys_s, ys_r, ag_s, ag_r):
    me = lax.axis_index('sp')
    n_chips = n_dev // 2
    core = lax.rem(me, 2)
    other = 1 - core
    chip = me // 2
    partner = me + 1 - 2 * core
    rchip, lchip, xchip = (lax.rem(chip + r, n_chips) for r in (1, 3, 2))
    right, left = rchip * 2 + core, lchip * 2 + core
    opposite = xchip * 2 + core
    chunks, n8 = o_buf.shape[0], o_buf.shape[1]
    rows = n8 * GROUP
    n_heads = n_dev * per
    dim = o_buf.shape[-1]
    width = per * dim
    half_o, half_y = o_buf.shape[4] // 2, rows // 2

    load_o = [pltpu.make_async_copy(o_hbm.at[k], o_buf.at[k], lsem.at[k]) for k in range(chunks)]
    load_w = pltpu.make_async_copy(wo_hbm, wo, lsem.at[chunks])
    for c in load_o:
        c.start()
    load_w.start()
    barrier = pltpu.get_barrier_semaphore()
    for r in range(1, n_dev):
        pl.semaphore_signal(barrier, inc=1, device_id={'sp': lax.rem(me + r, n_dev)}, device_id_type=MESH)
    pl.semaphore_wait(barrier, n_dev - 1)

    def remote(src, dst, s, r, dev):
        return pltpu.make_async_remote_copy(src, dst, s, r, device_id={'sp': dev}, device_id_type=MESH)

    stats = []
    for r in range(1, n_dev):
        dev = lax.rem(me + r, n_dev)
        c = remote(st_ref.at[dev], st_in.at[r - 1], st_s.at[r - 1], st_r.at[r - 1], dev)
        c.start()
        stats.append(c)
    for c in stats:
        c.wait_recv()
    mine = st_ref[0, :n_heads]
    top = mine
    for r in range(n_dev - 1):
        top = jnp.maximum(top, st_in[r, :n_heads])
    fac[...] = jnp.concatenate([jnp.exp2(mine - top), jnp.zeros((fac.shape[1] - n_heads, fac.shape[0]), F32)], axis=0).T
    total = jnp.zeros((8, top.shape[1]), F32)
    for d in range(n_dev):
        def term(st, top_d):
            return st[n_heads:n_heads + per] * jnp.exp2(st[per * d:per * (d + 1)] - top_d)
        top_d = top[per * d:per * (d + 1)]
        part = st_ref[d, n_heads:n_heads + per] * jnp.exp2(mine[per * d:per * (d + 1)] - top_d)
        for r in range(n_dev - 1):
            part += term(st_in[r], top_d)
        part = jnp.concatenate([part, jnp.ones((8 - per, top.shape[1]), F32)], axis=0)
        total = jnp.where(me == d, part, total)
    linv[...] = jnp.concatenate([total, jnp.ones((linv.shape[1] - 8, linv.shape[0]), F32)], axis=0).T

    class Reduce:
        def __init__(self, half, pair_src, pair, r1, l1, r2, l2, s, r):
            self.half, self.pair_src, self.pair = half, pair_src, pair
            self.r1, self.l1, self.r2, self.l2, self.s, self.r = r1, l1, r2, l2, s, r

        def copies(self, k):
            h = functools.partial(self.half, k)
            s, r = self.s, self.r
            return dict(
                pair=lambda: remote(self.pair_src(k), self.pair.at[k], s.at[k, 0], r.at[k, 0], partner),
                r1=lambda: remote(h(xchip, 0), self.r1.at[k], s.at[k, 1], r.at[k, 1], right),
                l1=lambda: remote(h(xchip, 1), self.l1.at[k], s.at[k, 2], r.at[k, 2], left),
                r2a=lambda: remote(h(rchip, 1), self.r2.at[k, 1], s.at[k, 3], r.at[k, 3], right),
                l2a=lambda: remote(h(lchip, 0), self.l2.at[k, 0], s.at[k, 4], r.at[k, 4], left),
                r2b=lambda: remote(h(rchip, 0), self.r2.at[k, 0], s.at[k, 5], r.at[k, 5], right),
                l2b=lambda: remote(h(lchip, 1), self.l2.at[k, 1], s.at[k, 6], r.at[k, 6], left),
            )

        def first(self, k, pair_half):
            c = self.copies(k)
            c['pair']().wait_recv()
            for x, g, name in ((xchip, 0, 'r1'), (xchip, 1, 'l1'), (rchip, 1, 'r2a'), (lchip, 0, 'l2a'),
                               (rchip, 0, None), (lchip, 1, None), (chip, 0, None), (chip, 1, None)):
                self.half(k, x, g)[...] += pair_half(k, x, g)[...]
                if name:
                    c[name]().start()

        def second(self, k):
            c = self.copies(k)
            c['r1']().wait_recv()
            self.half(k, rchip, 0)[...] += self.r1[k]
            c['r2b']().start()
            c['l1']().wait_recv()
            self.half(k, lchip, 1)[...] += self.l1[k]
            c['l2b']().start()

        def third(self, k):
            c = self.copies(k)
            for name in ('r2a', 'l2a', 'r2b', 'l2b'):
                c[name]().wait_recv()

        def drain(self, k):
            for c in self.copies(k).values():
                c().wait_send()

    red_o = Reduce(lambda k, x, g: o_buf.at[k, :, x, core, pl.ds(g * half_o, half_o), :],
                   lambda k: o_buf.at[k, :, :, other], o_pair, o_r1, o_l1, o_r2, o_l2, os_s, os_r)
    red_y = Reduce(lambda k, x, g: y_buf.at[k, core, x, pl.ds(g * half_y, half_y), :],
                   lambda k: y_buf.at[k, other], y_pair, y_r1, y_l1, y_r2, y_l2, ys_s, ys_r)

    def o_pair_half(k, x, g):
        return o_pair.at[k, :, x, pl.ds(g * half_o, half_o), :]

    def y_pair_half(k, x, g):
        return y_pair.at[k, x, pl.ds(g * half_y, half_y), :]

    def scale_o(k):
        load_o[k].wait()

        def one(t, carry):
            f = fac[pl.ds(pl.multiple_of(k * rows + t * GROUP, GROUP), GROUP), :]
            for h in range(n_heads):
                x, c, j = h // (2 * per), (h // per) % 2, h % per
                o_buf[k, t, x, c, j * GROUP:(j + 1) * GROUP, :] = o_buf[k, t, x, c, j * GROUP:(j + 1) * GROUP, :] * f[:, h:h + 1]
            return carry
        lax.fori_loop(0, n8, one, 0)
        red_o.copies(k)['pair']().start()

    def project(k):
        red_o.third(k)
        for t in range(n8):
            inv = linv[pl.ds(k * rows + t * GROUP, GROUP), :]
            for j in range(per):
                g, jj = j // (per // 2), j % (per // 2)
                sl = pl.ds(jj * GROUP, GROUP)
                v = (o_buf[k, t, chip, core, j * GROUP:(j + 1) * GROUP, :] + o_r2[k, g, t, sl, :]) + o_l2[k, g, t, sl, :]
                ob[t * GROUP:(t + 1) * GROUP, j * dim:(j + 1) * dim] = v / inv[:, j:j + 1]
        if k == 0:
            load_w.wait()
        a = ob[...].astype(BF16)
        for c in (other, core):
            def one(x, carry):
                col = pl.multiple_of((x * 2 + c) * width, width)
                y_buf[k, c, x] = jnp.dot(a, wo[:, pl.ds(col, width)], preferred_element_type=F32)
                return carry
            lax.fori_loop(0, n_chips, one, 0)
            if c is other:
                red_y.copies(k)['pair']().start()

    def y_block(k, dev, g=None):
        r = pl.ds(k * rows, rows) if g is None else pl.ds(k * rows + g * half_y, half_y)
        return y_ref.at[r, pl.ds(pl.multiple_of(dev * width, width), width)]

    def ag(k):
        s, r = ag_s, ag_r

        def to(block, i, dev):
            return lambda: remote(block, block, s.at[k, i], r.at[k, i], dev)
        return dict(
            own_r=to(y_block(k, me), 0, right), own_l=to(y_block(k, me), 1, left), own_p=to(y_block(k, me), 2, partner),
            fwd_r=to(y_block(k, left, 0), 3, right), fwd_l=to(y_block(k, right, 1), 4, left),
            left_p=to(y_block(k, left), 5, partner), right_p=to(y_block(k, right), 6, partner),
            opp_p0=to(y_block(k, opposite, 0), 7, partner), opp_p1=to(y_block(k, opposite, 1), 8, partner))

    def ag_in(k):
        s, r = ag_s, ag_r
        flip = lambda dev: dev + 1 - 2 * core

        def at(block, i):
            return lambda: remote(block, block, s.at[k, i], r.at[k, i], partner)
        return dict(
            left=at(y_block(k, left), 0), right=at(y_block(k, right), 1), own=at(y_block(k, partner), 2),
            opp0=at(y_block(k, opposite, 0), 3), opp1=at(y_block(k, opposite, 1), 4),
            left_p=at(y_block(k, flip(left)), 5), right_p=at(y_block(k, flip(right)), 6),
            opp_p0=at(y_block(k, flip(opposite), 0), 7), opp_p1=at(y_block(k, flip(opposite), 1), 8))

    def gather_start(k):
        red_y.third(k)
        for g in range(2):
            v = (y_buf[k, core, chip, g * half_y:(g + 1) * half_y, :] + y_r2[k, g]) + y_l2[k, g]
            y_block(k, me, g)[...] = v.astype(BF16)
        c = ag(k)
        for name in ('own_r', 'own_l', 'own_p'):
            c[name]().start()

    def gather_forward(k):
        c, i = ag(k), ag_in(k)
        i['left']().wait_recv()
        c['fwd_r']().start()
        c['left_p']().start()
        i['right']().wait_recv()
        c['fwd_l']().start()
        c['right_p']().start()

    def gather_opposite(k):
        c, i = ag(k), ag_in(k)
        for n in ('0', '1'):
            i['opp' + n]().wait_recv()
            c['opp_p' + n]().start()

    def gather_end(k):
        i = ag_in(k)
        for name in ('own', 'left_p', 'right_p', 'opp_p0', 'opp_p1'):
            i[name]().wait_recv()

    stages = [scale_o, lambda k: red_o.first(k, o_pair_half), red_o.second, project,
              lambda k: red_y.first(k, y_pair_half), red_y.second, gather_start, gather_forward, gather_opposite, gather_end]
    for t in range(chunks + len(stages) - 1):
        for s in reversed(range(len(stages))):
            if 0 <= t - s < chunks:
                stages[s](t - s)
    for c in stats:
        c.wait_send()
    for k in range(chunks):
        red_o.drain(k)
        red_y.drain(k)
        for c in ag(k).values():
            c().wait_send()


def solution(mesh):
    n_dev = mesh.shape['sp']

    def local_step(tokens, w_query, w_key, w_value, w_out, k_cache, v_cache, positions):
        n_rows, seq, dim = k_cache.shape
        d_model, q_width = w_query.shape
        n_heads = q_width // dim
        per = n_heads // n_dev
        width = 2 * dim
        n_tiles = q_width // width // 2
        depth = 3
        chunk = n_rows // CHUNKS
        n8 = chunk // GROUP
        dma = pltpu.SemaphoreType.DMA

        q, k_new, v_new = pl.pallas_call(
            functools.partial(project_kernel, n_tiles, depth),
            name='project',
            out_shape=[jax.ShapeDtypeStruct((n_heads, n_rows, dim), BF16)] + [jax.ShapeDtypeStruct((n_rows, dim), BF16)] * 2,
            in_specs=[VMEM, ANY, ANY, ANY], out_specs=[VMEM] * 3,
            scratch_shapes=[pltpu.VMEM((depth, d_model, width), BF16), pltpu.VMEM((2, d_model, dim), BF16),
                            dma((depth,)), dma((2,)), dma((n_tiles,)), dma((n_tiles,))],
            compiler_params=pltpu.CompilerParams(collective_id=0, has_side_effects=True, vmem_limit_bytes=20 * MIB),
        )(tokens, w_query, w_key, w_value)

        slots = 4
        n_blocks = n_rows // GROUP
        k_out, v_out, o_part, stats = pl.pallas_call(
            functools.partial(attend_kernel, n_heads, dim ** -0.5 * math.log2(math.e)),
            name='attend',
            out_shape=[jax.ShapeDtypeStruct(k_cache.shape, BF16), jax.ShapeDtypeStruct(v_cache.shape, BF16),
                       jax.ShapeDtypeStruct((n_blocks, n_heads * GROUP, dim), F32),
                       jax.ShapeDtypeStruct((n_dev, n_heads + 8, n_rows), F32)],
            in_specs=[SMEM, VMEM, VMEM, VMEM, ANY, ANY], out_specs=[ANY, ANY, ANY, VMEM],
            scratch_shapes=[pltpu.VMEM((slots, GROUP, seq, dim), BF16), pltpu.VMEM((slots, GROUP, seq, dim), BF16),
                            pltpu.VMEM((n_heads * GROUP, dim), F32), pltpu.VMEM((GROUP, n_heads, seq), F32), pltpu.VMEM((GROUP, n_heads, seq), BF16),
                            pltpu.VMEM((2, n_heads * GROUP, dim), F32),
                            pltpu.VMEM((n_rows, dim), F32), pltpu.VMEM((n_rows, dim), F32),
                            pltpu.VMEM((n_heads, n_rows), F32), pltpu.VMEM((n_heads, n_rows), F32),
                            dma((2, slots)), dma((2, slots)), dma((2,))],
            compiler_params=pltpu.CompilerParams(vmem_limit_bytes=24 * MIB),
        )(positions, q, k_new, v_new, k_cache, v_cache)

        n_chips = n_dev // 2
        o_view = o_part.reshape(CHUNKS, n8, n_chips, 2, per * GROUP, dim)
        ho, hy, out_w = per * GROUP // 2, chunk // 2, per * dim
        attn_out = pl.pallas_call(
            functools.partial(combine_kernel, n_dev, per),
            name='combine',
            out_shape=jax.ShapeDtypeStruct((n_rows, w_out.shape[1]), BF16),
            in_specs=[VMEM, ANY, ANY], out_specs=VMEM,
            scratch_shapes=[
                pltpu.VMEM(o_view.shape, F32), pltpu.VMEM(w_out.shape, BF16), pltpu.VMEM((n_dev - 1, n_heads + 8, n_rows), F32),
                pltpu.VMEM((n_rows, 128), F32), pltpu.VMEM((n_rows, 128), F32), pltpu.VMEM((chunk, out_w), F32),
                pltpu.VMEM((CHUNKS, n8, n_chips, per * GROUP, dim), F32),
                pltpu.VMEM((CHUNKS, n8, ho, dim), F32), pltpu.VMEM((CHUNKS, n8, ho, dim), F32),
                pltpu.VMEM((CHUNKS, 2, n8, ho, dim), F32), pltpu.VMEM((CHUNKS, 2, n8, ho, dim), F32),
                pltpu.VMEM((CHUNKS, 2, n_chips, chunk, out_w), F32), pltpu.VMEM((CHUNKS, n_chips, chunk, out_w), F32),
                pltpu.VMEM((CHUNKS, hy, out_w), F32), pltpu.VMEM((CHUNKS, hy, out_w), F32),
                pltpu.VMEM((CHUNKS, 2, hy, out_w), F32), pltpu.VMEM((CHUNKS, 2, hy, out_w), F32),
                dma((CHUNKS + 1,)), dma((n_dev - 1,)), dma((n_dev - 1,)),
                dma((CHUNKS, 7)), dma((CHUNKS, 7)), dma((CHUNKS, 7)), dma((CHUNKS, 7)), dma((CHUNKS, 9)), dma((CHUNKS, 9))],
            compiler_params=pltpu.CompilerParams(collective_id=1, has_side_effects=True, vmem_limit_bytes=36 * MIB),
        )(stats, o_view, w_out)
        return attn_out, k_out, v_out

    cache_spec = P('dp', 'sp', None)
    return jax.shard_map(local_step, mesh=mesh, in_specs=(P('dp', None), P(), P(), P(), P('sp', None), cache_spec, cache_spec, P('dp')),
                         out_specs=(P('dp', None), cache_spec, cache_spec), check_vma=False)
```
